512 devices in a mesh: blk: 512 (over x, y, z, core).
Axes of the slice: x: 4, y: 4, z: 16, core: 2. Of those that a mesh axis runs over, the one named last changes fastest.
Arguments:
- queries: bfloat16 [32768, 4096], P('blk'), may hold values from -200 to 200
- keys: bfloat16 [32768, 2048], P('blk'), may hold values from -8 to 8
- values: bfloat16 [32768, 2048], P('blk'), may hold values from -6 to 6
- doc_start: int32 [32768], P('blk'), may hold values from 0 to 32767, as said below
Outputs:
- attended: bfloat16 [32768, 4096], P('blk')
The draws below stay inside these ranges and needn't reach their ends.
Inputs may be any that keep to these rules, and one draw needn't show every extreme that they name: doc_start[i] is the first position of token i's document: nondecreasing, at most i, doc_start[doc_start[i]] = doc_start[i], and position 0 starts a document.
All inputs are finite; a program needn't handle non-finite values.
Results may differ from the reference program's by a relative error of at most 0.0034.
Values may be sent and summed in bfloat16 or wider, within the bound.
No kernel may reach another device: no remote copies, remote signals or barrier semaphores. Data moves between devices by JAX's collectives and lax.ppermute only.
A program may use at most 64 MiB of HBM per device.

```python
import jax
import jax.numpy as jnp
from jax import lax

HEADS = 16
KV_HEADS = 8
HD = 256
TOK_DEV = 64
HOPS = 4
GROUP = 2
TOKENS = 32768


def drawn_pair(key):
    base = jax.random.fold_in(key, 11)
    key_q, key_k = jax.random.split(base, 2)
    key_vectors = jax.random.normal(key_k, (TOKENS, KV_HEADS * HD), jnp.float32)
    query_vectors = jax.random.normal(key_q, (TOKENS, HEADS * HD), jnp.float32)
    query_vectors = jnp.clip(query_vectors, -5.0, 5.0)
    key_vectors = jnp.clip(key_vectors, -5.0, 5.0)
    return (query_vectors, key_vectors)


def draw_queries(key, part):
    query_vectors, key_vectors = drawn_pair(key)
    return query_vectors.astype(jnp.bfloat16)


def draw_keys(key, part):
    query_vectors, key_vectors = drawn_pair(key)
    return key_vectors.astype(jnp.bfloat16)


def draw_doc_start(key, part):
    base = jax.random.fold_in(key, 23)
    key_kind, key_cut = jax.random.split(base)
    nblocks = TOKENS // TOK_DEV
    longer = jax.random.randint(key_kind, (nblocks,), 0, 2)
    period = jnp.where(longer == 1, 6 * TOK_DEV, 24).astype(jnp.int32)
    period = jnp.repeat(period, TOK_DEV)
    draws = jax.random.randint(key_cut, (TOKENS,), 0, 1 << 30)
    positions = jnp.arange(TOKENS, dtype=jnp.int32)
    boundary = (draws % period == 0) | (positions == 0)
    marks = jnp.where(boundary, positions, jnp.int32(0))
    return lax.cummax(marks, axis=0).astype(jnp.int32)


def block_scale(key, dims, cuts, low, top_value):
    level, own = 1.0, jax.random.fold_in(key, 6)
    for position, shards_of in cuts:
        heights = jnp.exp(jax.random.uniform(jax.random.fold_in(own, position), (shards_of,), jnp.float32, low / len(cuts), top_value / len(cuts)))
        level = level * jnp.repeat(heights, dims[position] // shards_of).reshape([-1 if axis == position else 1 for axis in range(len(dims))])
    return level


def bell_draw(own_key, extent, scale, reach, pieces=(), kind=jnp.bfloat16):
    drawn = jax.random.normal(own_key, extent, jnp.float32) * scale
    if len(pieces) > 0:
        drawn = block_scale(own_key, extent, pieces, -0.22, 0.18) * drawn
    return jnp.clip(drawn, min=-reach, max=reach).astype(kind)


def setup_inputs(seed: int = 0) -> dict:
    streams_of = jax.random.split(jax.random.key(seed), 5)
    return {
        "queries": draw_queries(jax.random.fold_in(streams_of[4], 71), 0),
        "keys": draw_keys(jax.random.fold_in(streams_of[4], 71), 0),
        "values": bell_draw(streams_of[2], (TOKENS, KV_HEADS * HD), 1.0, 6.0, ((0, 512),)),
        "doc_start": draw_doc_start(jax.random.fold_in(streams_of[4], 71), 0),
    }


def reference(queries, keys, values, doc_start):
    window = HOPS * TOK_DEV
    span = window + TOK_DEV
    key_pad = jnp.pad(keys, ((window, 0), (0, 0)))
    value_pad = jnp.pad(values, ((window, 0), (0, 0)))

    def one_block(index):
        start = (index * TOK_DEV).astype(jnp.int32)
        query_block = lax.dynamic_slice(queries, (start, jnp.int32(0)), (TOK_DEV, HEADS * HD))
        query_block = query_block.astype(jnp.float32).reshape(TOK_DEV, KV_HEADS, GROUP, HD)
        key_block = lax.dynamic_slice(key_pad, (start, jnp.int32(0)), (span, KV_HEADS * HD))
        key_block = key_block.astype(jnp.float32).reshape(span, KV_HEADS, HD)
        value_block = lax.dynamic_slice(value_pad, (start, jnp.int32(0)), (span, KV_HEADS * HD))
        value_block = value_block.astype(jnp.float32).reshape(span, KV_HEADS, HD)
        scores = jnp.einsum('qgrd,kgd->grqk', query_block, key_block) * 0.0625
        q_pos = start + jnp.arange(TOK_DEV, dtype=jnp.int32)
        k_pos = start - window + jnp.arange(span, dtype=jnp.int32)
        starts = lax.dynamic_slice(doc_start, (start,), (TOK_DEV,))
        allowed = (k_pos[None, :] <= q_pos[:, None]) & (q_pos[:, None] - k_pos[None, :] < window) & (k_pos[None, :] >= starts[:, None])
        scores = jnp.where(allowed, scores, jnp.float32(-1e30))
        top = jnp.max(scores, axis=-1, keepdims=True)
        expo = jnp.exp(scores - top)
        total = jnp.sum(expo, axis=-1)
        weights = lax.optimization_barrier(expo.astype(jnp.bfloat16)).astype(jnp.float32)
        mixed = jnp.einsum('grqk,kgd->qgrd', weights, value_block)
        mixed = mixed / jnp.transpose(total, (2, 0, 1))[..., None]
        return mixed.reshape(TOK_DEV, HEADS * HD).astype(jnp.bfloat16)

    blocks = lax.map(one_block, jnp.arange(TOKENS // TOK_DEV, dtype=jnp.int32))
    return blocks.reshape(TOKENS, HEADS * HD)
```

```python
import jax
import jax.numpy as jnp
from jax import lax
from jax.experimental import pallas as pl
from jax.experimental.pallas import tpu as pltpu
from jax.sharding import PartitionSpec as P

HD = 256
HOPS = 4
NEG = -1e30
FAR = 1 << 30
F32 = jnp.float32
BF16 = jnp.bfloat16
VM = pl.BlockSpec(memory_space=pltpu.VMEM)
ANY = pl.BlockSpec(memory_space=pl.ANY)


def scores_of(q, keys, g):
    q2 = jnp.concatenate([q[:, (2 * g) * HD : (2 * g + 1) * HD], q[:, (2 * g + 1) * HD : (2 * g + 2) * HD]], axis=0)
    k2 = jnp.concatenate([k[:, g * HD : (g + 1) * HD] for k in keys], axis=0)
    return lax.dot_general(q2, k2, (((1,), (1,)), ((), ())), preferred_element_type=F32)


def near_scores(q, k0, ks, k1, k1s, out):
    for g in range(k0.shape[1] // HD):
        out[g] = scores_of(q, (k0, ks, k1, k1s), g)


def weigh(q, k2, k2s, near, v0, vs, v1, v1s, qpos, kpos, starts, w_far, acc, total):
    allowed = (kpos[...] <= qpos[...]) & (qpos[...] - kpos[...] < HOPS * q.shape[0]) & (kpos[...] >= starts[...])
    rows = q.shape[0]
    wide = near.shape[2]
    for g in range(k2.shape[1] // HD):
        far = scores_of(q, (k2, k2s), g)
        s = jnp.concatenate([near[g], far], axis=1) * 0.0625
        s = jnp.where(allowed, s, NEG)
        top = jnp.max(s, axis=1, keepdims=True)
        expo = jnp.exp(s - top)
        total[g] = jnp.broadcast_to(jnp.sum(expo, axis=1, keepdims=True), total.shape[1:])
        w = expo.astype(BF16)
        w_far[g] = w[:, wide:]
        v = jnp.concatenate([x[:, g * HD : (g + 1) * HD] for x in (v0, vs, v1, v1s)], axis=0)
        o = jnp.dot(w[:, :wide], v, preferred_element_type=F32)
        acc[:, (2 * g) * HD : (2 * g + 1) * HD] = o[:rows]
        acc[:, (2 * g + 1) * HD : (2 * g + 2) * HD] = o[rows:]


def finish(v2, v2s, w_far, acc, total, out):
    rows = acc.shape[0]
    for g in range(v2.shape[1] // HD):
        v = jnp.concatenate([x[:, g * HD : (g + 1) * HD] for x in (v2, v2s)], axis=0)
        o = jnp.dot(w_far[g], v, preferred_element_type=F32)
        t = total[g][:, :1]
        lo = slice((2 * g) * HD, (2 * g + 1) * HD)
        hi = slice((2 * g + 1) * HD, (2 * g + 2) * HD)
        out[:, lo] = ((acc[:, lo] + o[:rows]) / t[:rows]).astype(BF16)
        out[:, hi] = ((acc[:, hi] + o[rows:]) / t[rows:]).astype(BF16)


def call(body, out_shape, args, name):
    return pl.pallas_call(
        body,
        out_shape=out_shape,
        in_specs=[VM] * len(args),
        out_specs=jax.tree.map(lambda _: VM, out_shape),
        compiler_params=pltpu.CompilerParams(vmem_limit_bytes=12 << 20),
        name=name,
    )(*args)


def per_device(queries, keys, values, doc_start):
    n = lax.axis_size("blk")
    me = lax.axis_index("blk")
    rows = queries.shape[0]
    heads = keys.shape[1] // HD
    sds = jax.ShapeDtypeStruct
    chip = [(i, i + 2) for i in range(n - 2)]
    swap = [(i, i ^ 1) for i in range(n)]
    up = [(i, i + 1) for i in range(0, n, 2)]
    down = [(i + 1, i) for i in range(0, n, 2)]

    def send(x, route):
        return lax.ppermute(x, "blk", route)

    k1 = send(keys, chip)
    v1 = send(values, chip)
    ks = send(keys, up)
    vs = send(values, up)
    k2 = send(k1, chip)
    k1s = send(k1, swap)
    v2 = send(v1, chip)
    v1s = send(v1, swap)
    k2s = send(k2, down)
    v2s = send(v2, down)

    start = me * rows
    odd = me % 2 == 1
    bases = jnp.stack([
        start,
        jnp.where(odd, start - rows, FAR),
        start - 2 * rows,
        jnp.where(odd, start - 3 * rows, start - rows),
        start - 4 * rows,
        jnp.where(odd, FAR, start - 3 * rows),
    ]).astype(jnp.int32)
    kpos = (bases[:, None] + jnp.arange(rows, dtype=jnp.int32)[None, :]).reshape(1, 6 * rows)
    qpos = (start + jnp.arange(2 * rows, dtype=jnp.int32) % rows).reshape(2 * rows, 1)
    starts = jnp.concatenate([doc_start, doc_start]).reshape(2 * rows, 1)

    near = call(near_scores, sds((heads, 2 * rows, 4 * rows), F32), (queries, keys, ks, k1, k1s), "near_scores")
    w_far, acc, total = call(
        weigh,
        (sds((heads, 2 * rows, 2 * rows), BF16), sds((rows, queries.shape[1]), F32), sds((heads, 2 * rows, 128), F32)),
        (queries, k2, k2s, near, values, vs, v1, v1s, qpos, kpos, starts),
        "weigh",
    )
    return call(finish, sds(queries.shape, BF16), (v2, v2s, w_far, acc, total), "finish")


def solution(mesh):
    return jax.shard_map(
        per_device,
        mesh=mesh,
        in_specs=(P("blk", None), P("blk", None), P("blk", None), P("blk")),
        out_specs=P("blk", None),
        check_vma=False,
    )
```
